32 devices in a mesh: dp: 8 (over y, x, core), fsdp: 4 (over z).
Axes of the slice: x: 2, y: 2, z: 4, core: 2. Of those that a mesh axis runs over, the one named last changes fastest.
Arguments:
- tokens: bfloat16 [4096, 4096], P('dp'), may hold values from -6 to 6
- counts: int32 [8], P('dp'), may hold values from 256 to 512, as said below
- patch_index: int32 [4096], P('dp'), may hold values from 0 to 255
- clip_limit: float32 [], replicated, may hold values from 1024 to 8192
- norm_gain: float32 [4, 4096], replicated, may hold values from 0.25 to 1.75
- params: float32 [4, 4096, 4096], P(None, 'dp', 'fsdp'), may hold values from -0.09375 to 0.09375
- moments: float32 [4, 4096, 4096], P(None, 'dp', 'fsdp'), may hold values from -0.3 to 0.3
- seconds: float32 [4, 4096, 4096], P(None, 'dp', 'fsdp'), may hold values from 0.05 to 1
- gradients: float32 [4, 4096, 4096], P(None, 'dp', 'fsdp'), may hold values from -48 to 48
Outputs:
- params_new: float32 [4, 4096, 4096], P(None, 'dp', 'fsdp')
- moments_new: float32 [4, 4096, 4096], P(None, 'dp', 'fsdp')
- seconds_new: float32 [4, 4096, 4096], P(None, 'dp', 'fsdp')
- mixed: bfloat16 [4096, 4096], P('dp', 'fsdp')
The draws below stay inside these ranges and needn't reach their ends.
Inputs may be any that keep to these rules, and one draw needn't show every extreme that they name: `counts`: at most 512, reached on some index of dp in every draw.
All inputs are finite; a program needn't handle non-finite values.
Results may differ from the reference program's by a relative error of at most 0.0095.
Values may be sent and summed in bfloat16 or wider, within the bound.
A program may use at most 192 MiB of HBM per device.

```python
import math
import jax
import jax.numpy as jnp
from jax import lax

D = 4096
TOK_DEV = 512
LAYERS = 4
GRID = 16
STEP = 40
TOKENS = 4096
N_DP = 8


def draw_counts(key, part):
    drawn = jax.random.randint(key, (N_DP,), TOK_DEV // 2, TOK_DEV + 1)
    chosen = jax.random.randint(jax.random.fold_in(key, 3), (), 0, N_DP)
    return jnp.where(jnp.arange(N_DP) == chosen, TOK_DEV, drawn).astype(jnp.int32)


def draw_gradients(key, part):
    rising = jnp.arange(D, dtype=jnp.float32)[None, :, None] / D
    scaling = 1.0 + 2.0 * rising
    noise = jnp.clip(jax.random.normal(key, (LAYERS, D, D), jnp.float32), -6.0, 6.0)
    return scaling * noise


def with_ends(values, key, low, high):
    longest = values.shape.index(max(values.shape))
    spots = []
    for shift in (0, 1):
        where = [jax.random.randint(jax.random.fold_in(key, axis), (), 0, length) for axis, length in enumerate(values.shape)]
        where[longest] = (where[longest] + shift) % values.shape[longest]
        spots.append(tuple(where))
    return values.at[spots[0]].set(low).at[spots[1]].set(high)


def block_scale(own_key, shape, cuts, smallest, high):
    factor_of = 1.0
    for dim, shards_of in cuts:
        draws = jax.random.uniform(jax.random.fold_in(jax.random.fold_in(own_key, 6), dim), (shards_of,), jnp.float32, smallest / len(cuts), high / len(cuts))
        factor_of = factor_of * jnp.repeat(jnp.exp(draws), shape[dim] // shards_of).reshape((-1,) + (1,) * (len(shape) - 1 - dim))
    return factor_of


def normal_values(key, dims, deviation, limit, split=(), held_as=jnp.bfloat16):
    entries = jax.random.normal(key, dims, jnp.float32) * deviation
    if len(split) > 0:
        entries = block_scale(key, dims, split, -0.22, 0.18) * entries
    return jnp.clip(entries, min=-limit, max=limit).astype(held_as)


def setup_inputs(seed: int = 0) -> dict:
    seeds = jax.random.split(jax.random.key(seed), 10)
    tokens = normal_values(seeds[0], (TOKENS, D), 1.0, 6.0, ((0, 8),))
    counts = draw_counts(jax.random.fold_in(seeds[9], 71), 0)
    patch_index = with_ends(jax.random.randint(seeds[2], (TOKENS,), 0, GRID * GRID), jax.random.fold_in(seeds[2], 1), 0, (GRID * GRID) - 1).astype(jnp.int32)
    clip_limit = jnp.clip(jnp.exp(jax.random.uniform(seeds[3], (), jnp.float32, math.log(1024.0), math.log(8192.0))), 1024.0, 8192.0)
    norm_gain = jnp.clip(1.0 + 0.15 * jax.random.normal(seeds[4], (LAYERS, D), jnp.float32), 0.25, 1.75)
    params = normal_values(seeds[5], (LAYERS, D, D), D ** -0.5, 0.09375, ((1, 8), (2, 4)), jnp.float32)
    moments = normal_values(seeds[6], (LAYERS, D, D), 0.05, 0.3, ((1, 8), (2, 4)), jnp.float32)
    seconds = jnp.clip(jnp.exp(math.log(1.0) - 2.9957323 * jax.random.uniform(seeds[7], (LAYERS, D, D), jnp.float32) ** block_scale(seeds[7], (LAYERS, D, D), ((1, 8), (2, 4)), -0.2, 0.2)), 0.05, 1.0)
    gradients = draw_gradients(jax.random.fold_in(seeds[9], 71), 0)
    return dict(tokens=tokens, counts=counts, patch_index=patch_index, clip_limit=clip_limit, norm_gain=norm_gain, params=params, moments=moments, seconds=seconds, gradients=gradients)


beta_one = 0.9
beta_two = 0.95
adam_eps = 1e-08
learning_rate = 0.0024
weight_decay = 0.05
norm_eps = 1e-06

def position_code(patch_index):
    quarter = D // 4
    freqs = 1.0 / 10000.0 ** (jnp.arange(quarter, dtype=jnp.float32) / quarter)
    across = (patch_index // GRID).astype(jnp.float32)[:, None] * freqs[None, :]
    downward = (patch_index % GRID).astype(jnp.float32)[:, None] * freqs[None, :]
    return jnp.concatenate([jnp.sin(across), jnp.cos(across), jnp.sin(downward), jnp.cos(downward)], axis=1)

def layer_norm(stream, gain_row):
    centre = lax.optimization_barrier(jnp.mean(stream, axis=1, keepdims=True))
    shifted = stream - centre
    spread = lax.optimization_barrier(jnp.mean(shifted * shifted, axis=1, keepdims=True))
    return (shifted * lax.rsqrt(spread + norm_eps) * gain_row[None, :]).astype(jnp.bfloat16)

def adam_update(params, moments, seconds, gradients, factor):
    clipped = gradients * factor
    moments_new = beta_one * moments + (1.0 - beta_one) * clipped
    seconds_new = beta_two * seconds + (1.0 - beta_two) * clipped * clipped
    direction = moments_new / (1.0 - beta_one ** STEP) / (jnp.sqrt(seconds_new / (1.0 - beta_two ** STEP)) + adam_eps)
    params_new = params - learning_rate * (direction + weight_decay * params)
    return (params_new, moments_new, seconds_new)

def reference(tokens, counts, patch_index, clip_limit, norm_gain, params, moments, seconds, gradients):
    squares = jnp.sum(gradients * gradients)
    factor = jnp.minimum(1.0, clip_limit / (jnp.sqrt(squares) + 1e-06))
    params_new, moments_new, seconds_new = adam_update(params, moments, seconds, gradients, factor)
    weights = params_new.astype(jnp.bfloat16)
    slot = jnp.arange(TOKENS, dtype=jnp.int32) % TOK_DEV
    valid = (slot < jnp.repeat(counts, TOK_DEV, total_repeat_length=TOKENS))[:, None]
    stream = jnp.where(valid, tokens.astype(jnp.float32) + position_code(patch_index), 0.0)
    for current in range(LAYERS):
        normed = layer_norm(stream, norm_gain[current])
        branch = jnp.dot(normed, weights[current], preferred_element_type=jnp.float32).astype(jnp.bfloat16)
        stream = stream + branch.astype(jnp.float32)
    mixed = jnp.where(valid, stream, 0.0).astype(jnp.bfloat16)
    return (params_new, moments_new, seconds_new, mixed)
```

```python
import functools
import jax
import jax.numpy as jnp
from jax import lax
from jax.experimental import pallas as pl
from jax.experimental.pallas import tpu as pltpu
from jax.sharding import PartitionSpec as P

GRID = 16
STEP = 40

beta_one = 0.9
beta_two = 0.95
adam_eps = 1e-08
learning_rate = 0.0024
weight_decay = 0.05
norm_eps = 1e-06

MESH = pl.DeviceIdType.MESH
ANY = pl.BlockSpec(memory_space=pl.ANY)
VMEM = pl.BlockSpec(memory_space=pltpu.VMEM)
SMEM = pl.BlockSpec(memory_space=pltpu.SMEM)


def position_code(patch_index, width):
    quarter = width // 4
    freqs = 1.0 / 10000.0 ** (jnp.arange(quarter, dtype=jnp.float32) / quarter)
    across = (patch_index // GRID).astype(jnp.float32)[:, None] * freqs[None, :]
    downward = (patch_index % GRID).astype(jnp.float32)[:, None] * freqs[None, :]
    return jnp.concatenate(
        [jnp.sin(across), jnp.cos(across), jnp.sin(downward), jnp.cos(downward)], axis=1
    )


def adam_update(params, moments, seconds, gradients, factor):
    clipped = gradients * factor
    moments_new = beta_one * moments + (1.0 - beta_one) * clipped
    seconds_new = beta_two * seconds + (1.0 - beta_two) * clipped * clipped
    direction = (
        moments_new
        / (1.0 - beta_one**STEP)
        / (jnp.sqrt(seconds_new / (1.0 - beta_two**STEP)) + adam_eps)
    )
    params_new = params - learning_rate * (direction + weight_decay * params)
    return (params_new, moments_new, seconds_new)


def total_kernel(sizes, x_ref, o_ref, *scratch):
    names = ("dp", "fsdp")
    mid, got, send, recv = scratch[0], scratch[1:3], scratch[3:5], scratch[5:7]
    place = [lax.axis_index(name) for name in names]
    barrier = pltpu.get_barrier_semaphore()
    for axis in range(2):
        for step in range(1, sizes[axis]):
            pl.semaphore_signal(
                barrier,
                inc=1,
                device_id={names[axis]: lax.rem(place[axis] + step, sizes[axis])},
                device_id_type=MESH,
            )
    pl.semaphore_wait(barrier, sizes[0] + sizes[1] - 2)
    for axis in range(2):
        source = x_ref if axis == 0 else mid
        copies = []
        for step in range(1, sizes[axis]):
            copy = pltpu.make_async_remote_copy(
                src_ref=source,
                dst_ref=got[axis].at[place[axis]],
                send_sem=send[axis].at[step - 1],
                recv_sem=recv[axis].at[step - 1],
                device_id={names[axis]: lax.rem(place[axis] + step, sizes[axis])},
                device_id_type=MESH,
            )
            copy.start()
            copies.append(copy)
        got[axis][place[axis]] = source[...]
        for copy in copies:
            copy.wait()
        total = got[axis][0]
        for slot in range(1, sizes[axis]):
            total = total + got[axis][slot]
        if axis == 0:
            mid[...] = total
        else:
            o_ref[...] = total


def total_over_mesh(value, sizes):
    shape = (8, 128)
    total = pl.pallas_call(
        functools.partial(total_kernel, sizes),
        out_shape=jax.ShapeDtypeStruct(shape, jnp.float32),
        in_specs=[VMEM],
        out_specs=VMEM,
        scratch_shapes=[
            pltpu.VMEM(shape, jnp.float32),
            pltpu.VMEM((sizes[0],) + shape, jnp.float32),
            pltpu.VMEM((sizes[1],) + shape, jnp.float32),
        ]
        + [pltpu.SemaphoreType.DMA((max(size - 1, 1),)) for size in sizes] * 2,
        compiler_params=pltpu.CompilerParams(collective_id=0, has_side_effects=True),
        name="total",
    )(jnp.full(shape, value))
    return total[0, 0]


def layer_kernel(first, last, n, chunks, names, *refs):
    r = dict(zip(names, refs))
    place = lax.axis_index("fsdp")
    rows, width = r["stream"].shape
    cols = r["weights"].shape[1]
    part = rows // chunks
    depth = r["w"].shape[0] // 4

    def rows_of(c):
        return pl.ds(pl.multiple_of(c * part, part), part)

    def cols_of(owner):
        return pl.ds(pl.multiple_of(owner * cols, cols), cols)

    def take_stream(c):
        return pltpu.make_async_copy(
            r["stream"].at[rows_of(c)], r["s"].at[rows_of(c)], r["s_sem"].at[c]
        )

    def take_branch(c):
        return pltpu.make_async_copy(
            r["branch"].at[rows_of(c)], r["b"].at[rows_of(c)], r["b_sem"].at[c]
        )

    def take_weights(k):
        piece = pl.ds(k * depth, depth)
        return pltpu.make_async_copy(r["weights"].at[piece], r["w"].at[piece], r["w_sem"].at[k])

    def put_stream(c):
        return pltpu.make_async_copy(
            r["s"].at[rows_of(c)], r["stream_out"].at[rows_of(c)], r["so_sem"].at[c]
        )

    def put_own(c):
        return pltpu.make_async_copy(
            r["own"].at[rows_of(c)],
            r["branch_out"].at[rows_of(c), cols_of(place)],
            r["own_sem"].at[c],
        )

    def pass_on(way, hop, c):
        if hop == 0:
            owner = place
            source = r["own"].at[rows_of(c)]
        else:
            owner = place - hop if way == 0 else place + hop
            source = r["branch_out"].at[rows_of(c), cols_of(owner)]
        peer = lax.rem(place + 1, n) if way == 0 else lax.rem(place + n - 1, n)
        return pltpu.make_async_remote_copy(
            src_ref=source,
            dst_ref=r["branch_out"].at[rows_of(c), cols_of(owner)],
            send_sem=r["send"].at[way, hop, c],
            recv_sem=r["recv"].at[way, hop, c],
            device_id={"fsdp": peer},
            device_id_type=MESH,
        )

    def has_sent(way, hop):
        if way == 0:
            return jnp.logical_and(place < n - 1, place >= hop)
        return jnp.logical_and(place > 0, place + hop < n)

    def has_got(way, hop):
        return place >= hop + 1 if way == 0 else place + hop + 1 < n

    for c in range(chunks):
        take_stream(c).start()
        if not first:
            take_branch(c).start()
        if c == 0:
            for k in range(4):
                take_weights(k).start()

    if not last:
        barrier = pltpu.get_barrier_semaphore()
        for step in (1, n - 1):
            pl.semaphore_signal(
                barrier, inc=1, device_id={"fsdp": lax.rem(place + step, n)}, device_id_type=MESH
            )
        pl.semaphore_wait(barrier, 2)

    sub = 32
    tile = 256

    def chunk_body(c, carry):
        take_stream(c).wait()
        if not first:
            take_branch(c).wait()

        def norm_body(k, carry):
            at = pl.ds(pl.multiple_of(c * part + k * sub, sub), sub)
            x = r["s"][at]
            if not first:
                x = x + r["b"][at].astype(jnp.float32)
                r["s"][at] = x
            centre = jnp.sum(x, axis=1, keepdims=True) * (1.0 / width)
            shifted = x - centre
            spread = jnp.sum(shifted * shifted, axis=1, keepdims=True) * (1.0 / width)
            normed = shifted * lax.rsqrt(spread + norm_eps) * r["gain"][...]
            r["x"][pl.ds(pl.multiple_of(k * sub, sub), sub)] = normed.astype(jnp.bfloat16)
            return carry

        lax.fori_loop(0, part // sub, norm_body, 0)
        if "stream_out" in r:
            put_stream(c).start()

        @pl.when(c == 0)
        def _():
            for k in range(4):
                take_weights(k).wait()

        def dot_body(t, carry):
            at = pl.ds(pl.multiple_of(t * tile, tile), tile)
            out = jnp.dot(
                r["x"][...], r["w"][:, at], preferred_element_type=jnp.float32
            ).astype(jnp.bfloat16)
            if last:
                mine = pl.ds(pl.multiple_of(place * cols + t * tile, tile), tile)
                slot = c * part + lax.broadcasted_iota(jnp.int32, (part, tile), 0)
                total = r["s"][rows_of(c), mine] + out.astype(jnp.float32)
                total = jnp.where(slot < r["counts"][0], total, 0.0)
                r["mixed"][rows_of(c), at] = total.astype(jnp.bfloat16)
            else:
                r["own"][rows_of(c), at] = out
            return carry

        lax.fori_loop(0, cols // tile, dot_body, 0)
        if not last:
            for way in range(2):

                @pl.when(has_sent(way, 0))
                def _():
                    pass_on(way, 0, c).start()

            put_own(c).start()
        return carry

    lax.fori_loop(0, chunks, chunk_body, 0)
    if last:
        return

    for hop in range(n - 1):

        def forward_body(c, carry):
            for way in range(2):

                @pl.when(has_got(way, hop))
                def _():
                    pass_on(way, hop, c).wait_recv()

                if hop + 1 < n - 1:

                    @pl.when(has_sent(way, hop + 1))
                    def _():
                        pass_on(way, hop + 1, c).start()

            return carry

        lax.fori_loop(0, chunks, forward_body, 0)

    def finish_body(c, carry):
        put_own(c).wait()
        if "stream_out" in r:
            put_stream(c).wait()
        for hop in range(n - 1):
            for way in range(2):

                @pl.when(has_sent(way, hop))
                def _():
                    pass_on(way, hop, c).wait_send()

        return carry

    lax.fori_loop(0, chunks, finish_body, 0)


def run_layer(current, layers, n, stream, branch, gain, weights, counts):
    first, last = current == 0, current + 1 == layers
    rows, width = stream.shape
    cols = weights.shape[1]
    chunks = 2 if last else 4
    part = rows // chunks
    dma = pltpu.SemaphoreType.DMA
    names, args, specs = ["stream"], [stream], [ANY]
    if not first:
        names, args, specs = names + ["branch"], args + [branch], specs + [ANY]
    names, args, specs = (
        names + ["gain", "weights"],
        args + [gain, weights],
        specs + [VMEM, ANY],
    )
    if last:
        names, args, specs = names + ["counts"], args + [counts], specs + [SMEM]
        out_names, out_shape, out_specs = (
            ["mixed"],
            [jax.ShapeDtypeStruct((rows, cols), jnp.bfloat16)],
            [VMEM],
        )
    else:
        out_names, out_shape = ["branch_out"], [jax.ShapeDtypeStruct((rows, width), jnp.bfloat16)]
        if not first:
            out_names = out_names + ["stream_out"]
            out_shape = out_shape + [jax.ShapeDtypeStruct((rows, width), jnp.float32)]
        out_specs = [ANY] * len(out_names)
    scratch = {
        "s": pltpu.VMEM((rows, width), jnp.float32),
        "w": pltpu.VMEM(weights.shape, jnp.bfloat16),
        "x": pltpu.VMEM((part, width), jnp.bfloat16),
        "s_sem": dma((chunks,)),
        "w_sem": dma((4,)),
    }
    if not first:
        scratch["b"] = pltpu.VMEM((rows, width), jnp.bfloat16)
        scratch["b_sem"] = dma((chunks,))
    if not last:
        scratch["own"] = pltpu.VMEM((rows, cols), jnp.bfloat16)
        scratch["own_sem"] = dma((chunks,))
        scratch["send"] = dma((2, n - 1, chunks))
        scratch["recv"] = dma((2, n - 1, chunks))
        if not first:
            scratch["so_sem"] = dma((chunks,))
    size = rows * cols
    out = pl.pallas_call(
        functools.partial(
            layer_kernel, first, last, n, chunks, names + out_names + list(scratch)
        ),
        out_shape=out_shape,
        in_specs=specs,
        out_specs=out_specs,
        scratch_shapes=list(scratch.values()),
        compiler_params=pltpu.CompilerParams(
            collective_id=None if last else 1 + current,
            has_side_effects=not last,
            vmem_limit_bytes=63 * 2**20,
        ),
        cost_estimate=pl.CostEstimate(
            flops=2 * size * width,
            bytes_accessed=(40 if last else 240) * size,
            transcendentals=0,
        ),
        name="last_layer" if last else "layer_%d" % current,
    )(*args)
    if last:
        return None, None, out[0]
    return (stream if first else out[1]), out[0], None


def per_device(
    sizes,
    tokens,
    counts,
    patch_index,
    clip_limit,
    norm_gain,
    params,
    moments,
    seconds,
    gradients,
):
    layers = params.shape[0]
    squares = total_over_mesh(jnp.sum(gradients * gradients), sizes)
    factor = jnp.minimum(1.0, clip_limit / (jnp.sqrt(squares) + 1e-06))
    head = adam_update(params[0], moments[0], seconds[0], gradients[0], factor)[0]
    head = head.astype(jnp.bfloat16)
    later_factor, head, patch_index = lax.optimization_barrier((factor, head, patch_index))
    params_new, moments_new, seconds_new = adam_update(
        params, moments, seconds, gradients, later_factor
    )
    weights = lax.all_gather(head, "dp", axis=0, tiled=True)
    tok_rows = tokens.shape[0]
    valid = lax.broadcasted_iota(jnp.int32, (tok_rows, 1), 0) < counts[0]
    stream = jnp.where(
        valid, tokens.astype(jnp.float32) + position_code(patch_index, tokens.shape[1]), 0.0
    )
    branch = mixed = following = None
    for current in range(layers):
        if current + 1 < layers:
            piece = params_new[current + 1].astype(jnp.bfloat16)
            ready = stream if current == 0 else branch
            piece, weights, ready = lax.optimization_barrier((piece, weights, ready))
            stream, branch = (ready, None) if current == 0 else (stream, ready)
            following = lax.all_gather(piece, "dp", axis=0, tiled=True)
        stream, branch, mixed = run_layer(
            current,
            layers,
            sizes[1],
            stream,
            branch,
            norm_gain[current][None],
            weights,
            counts,
        )
        weights = following
    return (params_new, moments_new, seconds_new, mixed)


def solution(mesh):
    sizes = (mesh.shape["dp"], mesh.shape["fsdp"])
    weight = P(None, "dp", "fsdp")
    return jax.shard_map(
        functools.partial(per_device, sizes),
        mesh=mesh,
        in_specs=(P("dp", None), P("dp"), P("dp"), P(), P(), weight, weight, weight, weight),
        out_specs=(weight, weight, weight, P("dp", "fsdp")),
        check_vma=False,
    )
```

```python
import functools
import jax
import jax.numpy as jnp
from jax import lax
from jax.experimental import pallas as pl
from jax.experimental.pallas import tpu as pltpu
from jax.sharding import PartitionSpec as P

GRID = 16
STEP = 40

beta_one = 0.9
beta_two = 0.95
adam_eps = 1e-08
learning_rate = 0.0024
weight_decay = 0.05
norm_eps = 1e-06

MESH = pl.DeviceIdType.MESH
ANY = pl.BlockSpec(memory_space=pl.ANY)
VMEM = pl.BlockSpec(memory_space=pltpu.VMEM)
SMEM = pl.BlockSpec(memory_space=pltpu.SMEM)


def position_code(patch_index, width):
    quarter = width // 4
    freqs = 1.0 / 10000.0 ** (jnp.arange(quarter, dtype=jnp.float32) / quarter)
    across = (patch_index // GRID).astype(jnp.float32)[:, None] * freqs[None, :]
    downward = (patch_index % GRID).astype(jnp.float32)[:, None] * freqs[None, :]
    return jnp.concatenate(
        [jnp.sin(across), jnp.cos(across), jnp.sin(downward), jnp.cos(downward)], axis=1
    )


def adam_update(params, moments, seconds, gradients, factor):
    clipped = gradients * factor
    moments_new = beta_one * moments + (1.0 - beta_one) * clipped
    seconds_new = beta_two * seconds + (1.0 - beta_two) * clipped * clipped
    direction = (
        moments_new
        / (1.0 - beta_one**STEP)
        / (jnp.sqrt(seconds_new / (1.0 - beta_two**STEP)) + adam_eps)
    )
    params_new = params - learning_rate * (direction + weight_decay * params)
    return (params_new, moments_new, seconds_new)


def total_kernel(sizes, x_ref, o_ref, *scratch):
    names = ("dp", "fsdp")
    mid, got, send, recv = scratch[0], scratch[1:3], scratch[3:5], scratch[5:7]
    place = [lax.axis_index(name) for name in names]
    barrier = pltpu.get_barrier_semaphore()
    for axis in range(2):
        for step in range(1, sizes[axis]):
            pl.semaphore_signal(
                barrier,
                inc=1,
                device_id={names[axis]: lax.rem(place[axis] + step, sizes[axis])},
                device_id_type=MESH,
            )
    pl.semaphore_wait(barrier, sizes[0] + sizes[1] - 2)
    for axis in range(2):
        source = x_ref if axis == 0 else mid
        copies = []
        for step in range(1, sizes[axis]):
            copy = pltpu.make_async_remote_copy(
                src_ref=source,
                dst_ref=got[axis].at[place[axis]],
                send_sem=send[axis].at[step - 1],
                recv_sem=recv[axis].at[step - 1],
                device_id={names[axis]: lax.rem(place[axis] + step, sizes[axis])},
                device_id_type=MESH,
            )
            copy.start()
            copies.append(copy)
        got[axis][place[axis]] = source[...]
        for copy in copies:
            copy.wait()
        total = got[axis][0]
        for slot in range(1, sizes[axis]):
            total = total + got[axis][slot]
        if axis == 0:
            mid[...] = total
        else:
            o_ref[...] = total


def total_over_mesh(value, sizes):
    shape = (8, 128)
    total = pl.pallas_call(
        functools.partial(total_kernel, sizes),
        out_shape=jax.ShapeDtypeStruct(shape, jnp.float32),
        in_specs=[VMEM],
        out_specs=VMEM,
        scratch_shapes=[
            pltpu.VMEM(shape, jnp.float32),
            pltpu.VMEM((sizes[0],) + shape, jnp.float32),
            pltpu.VMEM((sizes[1],) + shape, jnp.float32),
        ]
        + [pltpu.SemaphoreType.DMA((max(size - 1, 1),)) for size in sizes] * 2,
        compiler_params=pltpu.CompilerParams(collective_id=0, has_side_effects=True),
        name="total",
    )(jnp.full(shape, value))
    return total[0, 0]


def layer_kernel(first, last, n, chunks, names, *refs):
    r = dict(zip(names, refs))
    place = lax.axis_index("fsdp")
    rows, width = r["stream"].shape
    cols = r["weights"].shape[1]
    part = rows // chunks
    half = cols // 2
    tile = min(256, half)
    tiles = cols // tile
    sub = 32

    def rows_of(c):
        return pl.ds(pl.multiple_of(c * part, part), part)

    def cols_of(owner):
        return pl.ds(pl.multiple_of(owner * cols, cols), cols)

    def take_stream(c):
        return pltpu.make_async_copy(
            r["stream"].at[rows_of(c)], r["s"].at[rows_of(c)], r["s_sem"].at[c]
        )

    def take_branch(c):
        return pltpu.make_async_copy(
            r["branch"].at[rows_of(c)], r["b"].at[rows_of(c)], r["b_sem"].at[c]
        )

    def take_weights(k):
        piece = pl.ds(pl.multiple_of(k * tile, tile), tile)
        return pltpu.make_async_copy(
            r["weights"].at[:, piece], r["w"].at[:, piece], r["w_sem"].at[k]
        )

    def put_stream(c):
        return pltpu.make_async_copy(
            r["s"].at[rows_of(c)], r["stream_out"].at[rows_of(c)], r["so_sem"].at[c]
        )

    def put_own(c):
        return pltpu.make_async_copy(
            r["own"].at[rows_of(c)],
            r["branch_out"].at[rows_of(c), cols_of(place)],
            r["own_sem"].at[c],
        )

    def pass_on(way, hop, c, side):
        owner = place - hop if way == 0 else place + hop
        target = r["branch_out"].at[
            rows_of(c), pl.ds(pl.multiple_of(owner * cols + side * half, half), half)
        ]
        source = r["own"].at[rows_of(c), pl.ds(side * half, half)] if hop == 0 else target
        peer = lax.rem(place + 1, n) if way == 0 else lax.rem(place + n - 1, n)
        return pltpu.make_async_remote_copy(
            src_ref=source,
            dst_ref=target,
            send_sem=r["send"].at[way, hop, 2 * c + side],
            recv_sem=r["recv"].at[way, hop, 2 * c + side],
            device_id={"fsdp": peer},
            device_id_type=MESH,
        )

    def has_sent(way, hop):
        if way == 0:
            return jnp.logical_and(place < n - 1, place >= hop)
        return jnp.logical_and(place > 0, place + hop < n)

    def has_got(way, hop):
        return place >= hop + 1 if way == 0 else place + hop + 1 < n

    def take_rows(c):
        take_stream(c).start()
        if not first:
            take_branch(c).start()

    take_rows(0)
    for k in range(tiles):
        take_weights(k).start()

    if not last:
        barrier = pltpu.get_barrier_semaphore()
        for step in (1, n - 1):
            pl.semaphore_signal(
                barrier, inc=1, device_id={"fsdp": lax.rem(place + step, n)}, device_id_type=MESH
            )
        pl.semaphore_wait(barrier, 2)

    def chunk_body(c, carry):
        take_stream(c).wait()
        if not first:
            take_branch(c).wait()

        def norm_body(k, carry):
            at = pl.ds(pl.multiple_of(c * part + k * sub, sub), sub)
            x = r["s"][at]
            if not first:
                x = x + r["b"][at].astype(jnp.float32)
                r["s"][at] = x
            centre = jnp.sum(x, axis=1, keepdims=True) * (1.0 / width)
            shifted = x - centre
            spread = jnp.sum(shifted * shifted, axis=1, keepdims=True) * (1.0 / width)
            normed = shifted * lax.rsqrt(spread + norm_eps) * r["gain"][...]
            r["x"][pl.ds(pl.multiple_of(k * sub, sub), sub)] = normed.astype(jnp.bfloat16)
            return carry

        lax.fori_loop(0, part // sub, norm_body, 0)
        if "stream_out" in r:
            put_stream(c).start()

        def dot_body(t, carry):
            @pl.when(c == 0)
            def _():
                take_weights(t).wait()

                @pl.when(t == tiles // 2 - 1)
                def _():
                    for later in range(1, chunks):
                        take_rows(later)

            at = pl.ds(pl.multiple_of(t * tile, tile), tile)
            out = jnp.dot(
                r["x"][...], r["w"][:, at], preferred_element_type=jnp.float32
            ).astype(jnp.bfloat16)
            if last:
                mine = pl.ds(pl.multiple_of(place * cols + t * tile, tile), tile)
                slot = c * part + lax.broadcasted_iota(jnp.int32, (part, tile), 0)
                total = r["s"][rows_of(c), mine] + out.astype(jnp.float32)
                total = jnp.where(slot < r["counts"][0], total, 0.0)
                r["mixed"][rows_of(c), at] = total.astype(jnp.bfloat16)
            else:
                r["own"][rows_of(c), at] = out
            return carry

        for side in range(2):
            lax.fori_loop(side * tiles // 2, (side + 1) * tiles // 2, dot_body, 0)
            if not last:
                for way in range(2):

                    @pl.when(has_sent(way, 0))
                    def _():
                        pass_on(way, 0, c, side).start()

        if not last:
            put_own(c).start()
        return carry

    lax.fori_loop(0, chunks, chunk_body, 0)
    if last:
        return

    for hop in range(n - 1):

        def forward_body(c, carry):
            for side in range(2):
                for way in range(2):

                    @pl.when(has_got(way, hop))
                    def _():
                        pass_on(way, hop, c, side).wait_recv()

                    if hop + 1 < n - 1:

                        @pl.when(has_sent(way, hop + 1))
                        def _():
                            pass_on(way, hop + 1, c, side).start()

            return carry

        lax.fori_loop(0, chunks, forward_body, 0)

    def finish_body(c, carry):
        put_own(c).wait()
        if "stream_out" in r:
            put_stream(c).wait()
        for hop in range(n - 1):
            for way in range(2):

                @pl.when(has_sent(way, hop))
                def _():
                    for side in range(2):
                        pass_on(way, hop, c, side).wait_send()

        return carry

    lax.fori_loop(0, chunks, finish_body, 0)


def run_layer(current, layers, n, stream, branch, gain, weights, counts):
    first, last = current == 0, current + 1 == layers
    rows, width = stream.shape
    cols = weights.shape[1]
    chunks = 4
    part = rows // chunks
    dma = pltpu.SemaphoreType.DMA
    names, args, specs = ["stream"], [stream], [ANY]
    if not first:
        names, args, specs = names + ["branch"], args + [branch], specs + [ANY]
    names, args, specs = (
        names + ["gain", "weights"],
        args + [gain, weights],
        specs + [VMEM, ANY],
    )
    if last:
        names, args, specs = names + ["counts"], args + [counts], specs + [SMEM]
        out_names, out_shape, out_specs = (
            ["mixed"],
            [jax.ShapeDtypeStruct((rows, cols), jnp.bfloat16)],
            [VMEM],
        )
    else:
        out_names, out_shape = ["branch_out"], [jax.ShapeDtypeStruct((rows, width), jnp.bfloat16)]
        if not first:
            out_names = out_names + ["stream_out"]
            out_shape = out_shape + [jax.ShapeDtypeStruct((rows, width), jnp.float32)]
        out_specs = [ANY] * len(out_names)
    scratch = {
        "s": pltpu.VMEM((rows, width), jnp.float32),
        "w": pltpu.VMEM(weights.shape, jnp.bfloat16),
        "x": pltpu.VMEM((part, width), jnp.bfloat16),
        "s_sem": dma((chunks,)),
        "w_sem": dma((cols // min(256, cols // 2),)),
    }
    if not first:
        scratch["b"] = pltpu.VMEM((rows, width), jnp.bfloat16)
        scratch["b_sem"] = dma((chunks,))
    if not last:
        scratch["own"] = pltpu.VMEM((rows, cols), jnp.bfloat16)
        scratch["own_sem"] = dma((chunks,))
        scratch["send"] = dma((2, n - 1, 2 * chunks))
        scratch["recv"] = dma((2, n - 1, 2 * chunks))
        if not first:
            scratch["so_sem"] = dma((chunks,))
    size = rows * cols
    out = pl.pallas_call(
        functools.partial(
            layer_kernel, first, last, n, chunks, names + out_names + list(scratch)
        ),
        out_shape=out_shape,
        in_specs=specs,
        out_specs=out_specs,
        scratch_shapes=list(scratch.values()),
        compiler_params=pltpu.CompilerParams(
            collective_id=None if last else 1 + current,
            has_side_effects=not last,
            vmem_limit_bytes=63 * 2**20,
        ),
        cost_estimate=pl.CostEstimate(
            flops=2 * size * width,
            bytes_accessed=(40 if last else 240) * size,
            transcendentals=0,
        ),
        name="last_layer" if last else "layer_%d" % current,
    )(*args)
    if last:
        return None, None, out[0]
    return (stream if first else out[1]), out[0], None


def per_device(
    sizes,
    tokens,
    counts,
    patch_index,
    clip_limit,
    norm_gain,
    params,
    moments,
    seconds,
    gradients,
):
    layers = params.shape[0]
    squares = total_over_mesh(jnp.sum(gradients * gradients), sizes)
    factor = jnp.minimum(1.0, clip_limit / (jnp.sqrt(squares) + 1e-06))
    head = adam_update(params[0], moments[0], seconds[0], gradients[0], factor)[0]
    head = head.astype(jnp.bfloat16)
    later_factor, head, patch_index = lax.optimization_barrier((factor, head, patch_index))
    params_new, moments_new, seconds_new = adam_update(
        params, moments, seconds, gradients, later_factor
    )
    weights = lax.all_gather(head, "dp", axis=0, tiled=True)
    tok_rows = tokens.shape[0]
    valid = lax.broadcasted_iota(jnp.int32, (tok_rows, 1), 0) < counts[0]
    stream = jnp.where(
        valid, tokens.astype(jnp.float32) + position_code(patch_index, tokens.shape[1]), 0.0
    )
    branch = mixed = following = None
    for current in range(layers):
        if current + 1 < layers:
            piece = params_new[current + 1].astype(jnp.bfloat16)
            ready = stream if current == 0 else branch
            piece, weights, ready = lax.optimization_barrier((piece, weights, ready))
            stream, branch = (ready, None) if current == 0 else (stream, ready)
            following = lax.all_gather(piece, "dp", axis=0, tiled=True)
        stream, branch, mixed = run_layer(
            current,
            layers,
            sizes[1],
            stream,
            branch,
            norm_gain[current][None],
            weights,
            counts,
        )
        weights = following
    return (params_new, moments_new, seconds_new, mixed)


def solution(mesh):
    sizes = (mesh.shape["dp"], mesh.shape["fsdp"])
    weight = P(None, "dp", "fsdp")
    return jax.shard_map(
        functools.partial(per_device, sizes),
        mesh=mesh,
        in_specs=(P("dp", None), P("dp"), P("dp"), P(), P(), weight, weight, weight, weight),
        out_specs=(weight, weight, weight, P("dp", "fsdp")),
        check_vma=False,
    )
```
